256 devices in a mesh: dp: 64 (over y, z, core), expert: 4 (over x).
Axes of the slice: x: 4, y: 4, z: 8, core: 2. Of those that a mesh axis runs over, the one named last changes fastest.
Arguments:
- gradients: bfloat16 [64, 1024, 128, 128], P('dp', 'expert'), may hold values from -600 to 600
- owner_table: int32 [4, 256], P('expert'), may hold values from 0 to 255, as said below
- step_count: int32 [1], replicated, may hold values from 1 to 8
- master: float32 [1024, 128, 128], P(('dp', 'expert')), may hold values from -0.078125 to 0.078125
- first_code: bfloat16 [1024, 128, 128], P(('dp', 'expert')), may hold values from -1 to 1
- first_scale: float32 [1024], P(('dp', 'expert')), may hold values from 0.1 to 1
- first_power: float32 [1024], P(('dp', 'expert')), may hold values from 1 to 3
- second_code: bfloat16 [1024, 128, 128], P(('dp', 'expert')), may hold values from 0.0099487305 to 1
- second_scale: float32 [1024], P(('dp', 'expert')), may hold values from 0.1 to 2
- second_power: float32 [1024], P(('dp', 'expert')), may hold values from 1 to 3
Outputs:
- new_master: float32 [1024, 128, 128], P(('dp', 'expert'))
- new_first_code: bfloat16 [1024, 128, 128], P(('dp', 'expert'))
- new_first_scale: float32 [1024], P(('dp', 'expert'))
- new_first_power: float32 [1024], P(('dp', 'expert'))
- new_second_code: bfloat16 [1024, 128, 128], P(('dp', 'expert'))
- new_second_scale: float32 [1024], P(('dp', 'expert'))
- new_second_power: float32 [1024], P(('dp', 'expert'))
- weight_code: bfloat16 [1024, 128, 128], P('dp')
- weight_scale: bfloat16 [1024], P('dp')
The draws below stay inside these ranges and needn't reach their ends.
Inputs may be any that keep to these rules, and one draw needn't show every extreme that they name: `owner_table`: each row is a permutation of 0 to 255.
All inputs are finite; a program needn't handle non-finite values. Where the reference program divides by a largest or mean magnitude, that divisor is 1e-20 or more.
Results may differ from the reference program's by a relative error of at most 0.009.
Values may be sent and summed in bfloat16 or wider, within the bound.
No kernel may reach another device: no remote copies, remote signals or barrier semaphores. Data moves between devices by JAX's collectives and lax.ppermute only.
A program may use at most 128 MiB of HBM per device.

```python
import math
import jax
import jax.numpy as jnp
from jax import lax

D = 6144
TILE = 128
OWN = 4
BLOCK = 256
TILES = 1024


def owner_rows(key):
    block_count = TILES // BLOCK
    subkeys = jax.random.split(key, block_count)

    def permute_row(subkey):
        return jax.random.permutation(subkey, BLOCK)
    return jax.vmap(permute_row)(subkeys).astype(jnp.int32)


def draw_owner_table(key, part):
    return owner_rows(jax.random.fold_in(key, 11))


def draw_gradients(key, part):
    owner_perm = owner_rows(jax.random.fold_in(key, 11))
    block_count = TILES // BLOCK
    rank_count = BLOCK // OWN
    row_ids = jnp.arange(block_count, dtype=jnp.int32)[:, None]
    slot_of = jnp.zeros((block_count, BLOCK), jnp.int32).at[row_ids, owner_perm].set(jnp.arange(BLOCK, dtype=jnp.int32)[None, :])
    owner_rank = (slot_of // OWN).reshape(TILES).astype(jnp.float32)
    rising = 1.0 + 2.0 * owner_rank / max(rank_count - 1, 1)
    tile_gain = rising * jnp.power(10.0, jax.random.uniform(jax.random.fold_in(key, 2), (TILES,), jnp.float32))
    replica_gain = jnp.power(10.0, jax.random.uniform(jax.random.fold_in(key, 3), (rank_count, TILES), jnp.float32, -0.5, 0.5))
    full_shape = (rank_count, TILES, TILE, TILE)
    values = jnp.clip(jax.random.normal(jax.random.fold_in(key, 4), full_shape, jnp.float32), -4.0, 4.0)
    scaled = values * tile_gain[None, :, None, None] * replica_gain[:, :, None, None]
    return scaled.astype(jnp.bfloat16)


def steps_of(own_key, dims, shards, smallest, high):
    gain = 1.0
    for position, blocks in shards:
        steps = jax.random.uniform(jax.random.fold_in(jax.random.fold_in(own_key, 6), position), (blocks,), jnp.float32, smallest / len(shards), high / len(shards))
        gain = gain * jnp.repeat(jnp.exp(steps), dims[position] // blocks).reshape((-1,) + (1,) * (len(dims) - 1 - position))
    return gain


def bell_draw(rng, shape, scale, most, shards=(), held_as=jnp.bfloat16):
    values = scale * jax.random.normal(rng, shape, jnp.float32)
    if shards:
        values = values * steps_of(rng, shape, shards, -0.22, 0.18)
    return jnp.clip(values, -most, most).astype(held_as)


def setup_inputs(seed: int = 0) -> dict:
    streams_of = jax.random.split(jax.random.key(seed), 11)
    gradients = draw_gradients(jax.random.fold_in(streams_of[10], 71), 0)
    owner_table = draw_owner_table(jax.random.fold_in(streams_of[10], 71), 0)
    step_count = jax.random.randint(streams_of[2], (1,), 1, 9).astype(jnp.int32)
    master = bell_draw(streams_of[3], (TILES, TILE, TILE), D ** -0.5, 0.078125, ((0, 256),), jnp.float32)
    first_code = jnp.clip(jax.random.uniform(streams_of[4], (TILES, TILE, TILE), jnp.float32, -1.0, 1.0) * steps_of(streams_of[4], (TILES, TILE, TILE), ((0, 256),), -0.4, 0.0), -1.0, 1.0).astype(jnp.bfloat16)
    first_scale = jnp.clip(jnp.exp(math.log(1.0) - 2.3025851 * jax.random.uniform(streams_of[5], (TILES,), jnp.float32) ** steps_of(streams_of[5], (TILES,), ((0, 256),), -0.2, 0.2)), 0.1, 1.0)
    first_power = jnp.clip(1.0 + 2.0 * jax.random.uniform(streams_of[6], (TILES,), jnp.float32) ** steps_of(streams_of[6], (TILES,), ((0, 256),), -0.2, 0.2), 1.0, 3.0)
    second_code = jnp.clip(jnp.exp(math.log(1.0) - 4.61031033 * jax.random.uniform(streams_of[7], (TILES, TILE, TILE), jnp.float32) ** steps_of(streams_of[7], (TILES, TILE, TILE), ((0, 256),), -0.2, 0.2)), 0.0099487305, 1.0).astype(jnp.bfloat16)
    second_scale = jnp.clip(jnp.exp(math.log(2.0) - 2.9957323 * jax.random.uniform(streams_of[8], (TILES,), jnp.float32) ** steps_of(streams_of[8], (TILES,), ((0, 256),), -0.2, 0.2)), 0.1, 2.0)
    second_power = jnp.clip(1.0 + 2.0 * jax.random.uniform(streams_of[9], (TILES,), jnp.float32) ** steps_of(streams_of[9], (TILES,), ((0, 256),), -0.2, 0.2), 1.0, 3.0)
    return dict(gradients=gradients, owner_table=owner_table, step_count=step_count, master=master, first_code=first_code, first_scale=first_scale, first_power=first_power, second_code=second_code, second_scale=second_scale, second_power=second_power)


BETA_ONE = 0.9
BETA_TWO = 0.95
LEARN_RATE = 0.01
WEIGHT_DECAY = 0.1
CLIP_RMS = 0.5
LOG_SPAN = 4.0
EPSILON = 1e-06
ADAM_EPS = 1e-08

def decode_moment(code, scale, power):
    values = code.astype(jnp.float32)
    magnitude = jnp.power(jnp.abs(values), 1.0 / power[:, None, None])
    return scale[:, None, None] * jnp.sign(values) * magnitude

def encode_moment(values):
    absval = jnp.abs(values)
    largest = lax.optimization_barrier(jnp.max(absval, axis=(1, 2)))
    average = lax.optimization_barrier(jnp.mean(absval, axis=(1, 2)))
    power = jnp.clip(LOG_SPAN / jnp.log(1.0 + largest / (average + EPSILON)), 1.0, 3.0)
    scale = largest + EPSILON
    scaled = absval / scale[:, None, None]
    coded = (jnp.sign(values) * jnp.power(scaled, power[:, None, None])).astype(jnp.bfloat16)
    return (coded, scale, power)

def finish(owned_grad, total_sq, numel, step_count, master, first_code, first_scale, first_power, second_code, second_scale, second_power):
    clip_factor = jnp.minimum(1.0, CLIP_RMS / jnp.sqrt(total_sq / numel + EPSILON))
    grad = owned_grad * clip_factor
    first_old = decode_moment(first_code, first_scale, first_power)
    second_old = decode_moment(second_code, second_scale, second_power)
    first = BETA_ONE * first_old + (1.0 - BETA_ONE) * grad
    second = BETA_TWO * second_old + (1.0 - BETA_TWO) * grad * grad
    tcount = step_count[0].astype(jnp.float32)
    bias_one = 1.0 - jnp.power(BETA_ONE, tcount)
    bias_two = 1.0 - jnp.power(BETA_TWO, tcount)
    update = first / bias_one / (jnp.sqrt(second / bias_two) + ADAM_EPS)
    new_master = master - LEARN_RATE * (update + WEIGHT_DECAY * master)
    first_out = encode_moment(first)
    second_out = encode_moment(second)
    weight_scale = (lax.optimization_barrier(jnp.max(jnp.abs(new_master), axis=(1, 2))) + EPSILON).astype(jnp.bfloat16)
    weight_code = (new_master / weight_scale.astype(jnp.float32)[:, None, None]).astype(jnp.bfloat16)
    return (new_master, first_out, second_out, weight_code, weight_scale)

def add_replica(running, replica):
    return (running + replica.astype(jnp.float32), None)

def reference(gradients, owner_table, step_count, master, first_code, first_scale, first_power, second_code, second_scale, second_power):
    block_size = owner_table.shape[1]
    expert_count = owner_table.shape[0]
    rank_count = block_size // OWN
    summed = lax.scan(add_replica, jnp.zeros(gradients.shape[1:], jnp.float32), gradients)[0]
    rank_ids = jnp.arange(rank_count, dtype=jnp.int32)[:, None, None]
    experts = jnp.arange(expert_count, dtype=jnp.int32)[None, :, None]
    within = jnp.arange(OWN, dtype=jnp.int32)[None, None, :]
    natural = experts * block_size + owner_table[experts, rank_ids * OWN + within]
    owned_grad = jnp.take(summed, natural.reshape(-1).astype(jnp.int32), axis=0)
    total_sq = jnp.sum(summed * summed)
    numel = float(master.shape[0] * TILE * TILE)
    new_master, first_out, second_out, weight_code, weight_scale = finish(owned_grad, total_sq, numel, step_count, master, first_code, first_scale, first_power, second_code, second_scale, second_power)
    return (new_master, first_out[0], first_out[1], first_out[2], second_out[0], second_out[1], second_out[2], weight_code, weight_scale)
```

```python
import jax
import jax.numpy as jnp
from jax import lax
from jax.experimental import pallas as pl
from jax.experimental.pallas import tpu as pltpu
from jax.sharding import Mesh
from jax.sharding import PartitionSpec as P

DP = ("y", "zh", "zl", "core")
Z = ("zh", "zl")
EVERY = ("y", "zh", "zl", "core", "expert")
DP_EXPERT = EVERY

OWN = 4
BETA_ONE = 0.9
BETA_TWO = 0.95
LEARN_RATE = 0.01
WEIGHT_DECAY = 0.1
CLIP_RMS = 0.5
LOG_SPAN = 4.0
EPSILON = 1e-06
ADAM_EPS = 1e-08

VMEM = pltpu.VMEM
SMEM = pltpu.SMEM

Y_EVEN = [(i, i ^ 1) for i in range(4)]
Y_ODD = [(i, i ^ 3) for i in range(4)]
Z_EVEN = [(i, i ^ 1) for i in range(8)]
Z_ODD = [(i, (i + 1) % 8 if i % 2 else (i - 1) % 8) for i in range(8)]

STEPS = (
    (("y", Y_EVEN), (Z, Z_EVEN), ("y", Y_ODD)),
    (("y", Y_ODD), (Z, Z_ODD), ("y", Y_EVEN)),
    ((Z, Z_EVEN), ("y", Y_EVEN), ("y", Y_ODD)),
    ((Z, Z_ODD), ("y", Y_ODD), ("y", Y_EVEN)),
)


def shifted(count, by):
    return [(i, (i + by) % count) for i in range(count)]


def owner_of(k, place, y, zh, zl):
    bits = ((place >> 4) & 1, (place >> 3) & 1, (place >> 2) & 1)
    shift = place & 3
    for bit, (axis, pairs) in zip(bits, STEPS[k]):
        goes = 1 - bit
        if axis == "y":
            y = y ^ (goes * (1 if pairs is Y_EVEN else 3))
        else:
            if pairs is Z_ODD:
                zh = (zh + goes * (2 * zl - 1)) & 3
            zl = zl ^ goes
    return y, (zh + shift) & 3, zl


def pick_kernel(where, table, grads, *rest):
    outs, (held, loaded, stored) = rest[:OWN], rest[OWN:]
    y, zh, zl, core = where[0], where[1], where[2], where[3]
    count = held.shape[1]

    for k in range(OWN):

        def load(place, _, k=k):
            oy, ozh, ozl = owner_of(k, place, y, zh, zl)
            slot = ((((oy * 4 + ozh) * 2 + ozl) * 2) + core) * OWN + k
            pltpu.make_async_copy(
                grads.at[table[slot]], held.at[k, place], loaded.at[k]
            ).start()
            return 0

        lax.fori_loop(0, count, load, 0, unroll=8)
    for k in range(OWN):
        pltpu.make_async_copy(outs[k], held.at[k], loaded.at[k]).wait()
        pltpu.make_async_copy(held.at[k], outs[k], stored.at[k]).start()
    for k in range(OWN):
        pltpu.make_async_copy(held.at[k], outs[k], stored.at[k]).wait()


def pick(where, table, grads):
    tile = grads.shape[1:]
    count = grads.shape[0] // (2 * OWN)
    return pl.pallas_call(
        pick_kernel,
        out_shape=[jax.ShapeDtypeStruct((count, *tile), grads.dtype)] * OWN,
        in_specs=[
            pl.BlockSpec(memory_space=SMEM),
            pl.BlockSpec(memory_space=SMEM),
            pl.BlockSpec(memory_space=pl.ANY),
        ],
        out_specs=[pl.BlockSpec(memory_space=pl.ANY)] * OWN,
        scratch_shapes=[
            VMEM((OWN, count, *tile), grads.dtype),
            pltpu.SemaphoreType.DMA((OWN,)),
            pltpu.SemaphoreType.DMA((OWN,)),
        ],
        name="pick",
    )(where, table, grads)


def root(magnitude, power):
    return jnp.exp(jnp.log(magnitude) * power)


def decode_kernel(fs, fp, ss, sp, master, first_code, second_code, out):
    for i in range(OWN):
        out[i] = master[i]
        for base, code, scale, power in ((OWN, first_code, fs, fp), (2 * OWN, second_code, ss, sp)):
            values = code[i].astype(jnp.float32)
            old = scale[i] * root(jnp.abs(values), 1.0 / jnp.full(values.shape, power[i]))
            out[base + i] = jnp.where(values < 0, -old, old)


def decode(fs, fp, ss, sp, master, first_code, second_code):
    return pl.pallas_call(
        decode_kernel,
        out_shape=jax.ShapeDtypeStruct((3 * OWN, *master.shape[1:]), jnp.float32),
        in_specs=[pl.BlockSpec(memory_space=SMEM)] * 4 + [pl.BlockSpec(memory_space=VMEM)] * 3,
        out_specs=pl.BlockSpec(memory_space=VMEM),
        name="decode",
    )(fs, fp, ss, sp, master, first_code, second_code)


def total_kernel(*refs):
    parts, (owned, row) = refs[:-2], refs[-2:]
    squares = jnp.zeros((1, owned.shape[-1]), jnp.float32)
    for k in range(OWN):
        total = parts[k][...]
        for received in parts[OWN:]:
            total = total + received[k].astype(jnp.float32)
        owned[k] = total
        squares = squares + jnp.sum(total * total, axis=0, keepdims=True)
    row[...] = jnp.broadcast_to(squares[None], row.shape)


def total(rests, received, devices):
    tile = rests[0].shape
    return pl.pallas_call(
        total_kernel,
        out_shape=[
            jax.ShapeDtypeStruct((OWN, *tile), jnp.float32),
            jax.ShapeDtypeStruct((devices, 1, tile[-1]), jnp.float32),
        ],
        in_specs=[pl.BlockSpec(memory_space=VMEM)] * (len(rests) + len(received)),
        out_specs=[pl.BlockSpec(memory_space=VMEM)] * 2,
        name="total",
    )(*rests, *received)


def encode(values, code, scales, powers, i):
    absval = jnp.abs(values)
    largest = jnp.max(absval)
    average = jnp.sum(absval) / float(values.shape[0] * values.shape[1])
    ratio = jnp.full((8, 128), largest) / (jnp.full((8, 128), average) + EPSILON)
    power = jnp.max(jnp.clip(LOG_SPAN / jnp.log(1.0 + ratio), 1.0, 3.0))
    scale = largest + EPSILON
    scales[i] = scale
    powers[i] = power
    coded = root(absval / scale, power)
    code[i] = jnp.where(values < 0, -coded, coded).astype(code.dtype)


def finish_kernel(
    numel, where, step, squares, *refs
):
    grads, states = refs[:4], refs[4:8]
    (new_master, fcode, fscale, fpower, scode, sscale, spower, wcode, wscale) = refs[8:]
    total_sq = jnp.sum(jnp.sum(squares[...], axis=0))
    mean_sq = jnp.full((8, 128), total_sq / numel + EPSILON)
    clip = jnp.max(jnp.minimum(1.0, CLIP_RMS / jnp.sqrt(mean_sq)))
    steps = jnp.full((8, 128), step[0]).astype(jnp.float32)
    bias_one = jnp.max(1.0 - jnp.exp(steps * jnp.log(jnp.full((8, 128), BETA_ONE))))
    bias_two = jnp.max(1.0 - jnp.exp(steps * jnp.log(jnp.full((8, 128), BETA_TWO))))
    for shift in range(4):
        base = ((where[4] - shift) & 3) * OWN
        for k in range(OWN):
            state = states[shift]
            master = state[k]
            grad = grads[shift][k] * clip
            first = BETA_ONE * state[OWN + k] + (1.0 - BETA_ONE) * grad
            second = BETA_TWO * state[2 * OWN + k] + (1.0 - BETA_TWO) * grad * grad
            update = first / bias_one / (jnp.sqrt(second / bias_two) + ADAM_EPS)
            moved = master - LEARN_RATE * (update + WEIGHT_DECAY * master)
            if shift == 0:
                new_master[k] = moved
                encode(first, fcode, fscale, fpower, k)
                encode(second, scode, sscale, spower, k)
            largest = jnp.max(jnp.abs(moved)) + EPSILON
            scale = jnp.full((8, 128), largest).astype(jnp.bfloat16).astype(jnp.float32)
            scale = jnp.max(scale)
            wscale[base + k] = scale
            wcode[base + k] = (moved / scale).astype(wcode.dtype)


def finish(numel, where, step, squares, grads, states):
    tile = grads[0].shape[1:]
    f32, bf16 = jnp.float32, jnp.bfloat16

    def body(*refs):
        finish_kernel(numel, *refs)

    shapes = [
        ((OWN, *tile), f32, VMEM),
        ((OWN, *tile), bf16, VMEM),
        ((OWN,), f32, SMEM),
        ((OWN,), f32, SMEM),
        ((OWN, *tile), bf16, VMEM),
        ((OWN,), f32, SMEM),
        ((OWN,), f32, SMEM),
        ((4 * OWN, *tile), bf16, VMEM),
        ((4 * OWN,), f32, SMEM),
    ]
    return pl.pallas_call(
        body,
        out_shape=[jax.ShapeDtypeStruct(s, d) for s, d, _ in shapes],
        in_specs=[pl.BlockSpec(memory_space=SMEM)] * 2 + [pl.BlockSpec(memory_space=VMEM)] * 9,
        out_specs=[pl.BlockSpec(memory_space=m) for _, _, m in shapes],
        name="finish",
    )(where, step, squares, *grads, *states)


def on_device(
    gradients,
    owner_table,
    step_count,
    master,
    first_code,
    first_scale,
    first_power,
    second_code,
    second_scale,
    second_power,
):
    f32, bf16 = jnp.float32, jnp.bfloat16
    devices = 256
    numel = float(devices * master.size)
    place = [lax.axis_index(a) for a in ("y", "zh", "zl", "core", "expert")]
    table = owner_table[0]
    grads = gradients[0]
    mine = jnp.stack(place).astype(jnp.int32)
    theirs = jnp.stack(place[:3] + [1 - place[3], place[4]]).astype(jnp.int32)

    leaving = pick(theirs, table, grads)
    from_core = [lax.ppermute(t, "core", [(0, 1), (1, 0)]) for t in leaving]
    kept = pick(mine, table, grads)

    state = decode(
        first_scale, first_power, second_scale, second_power, master, first_code, second_code
    )
    states = [state] + [lax.ppermute(state, "expert", shifted(4, s)) for s in (1, 2, 3)]

    held = [[kept[k], from_core[k]] for k in range(OWN)]

    def added(k, start, stop):
        longest = held[k][0].shape[0]
        return sum(
            p[p.shape[0] - longest + start : p.shape[0] - longest + stop].astype(f32)
            for p in held[k]
        )

    start, size = 0, 16
    for step in range(3):
        arrived = []
        for k in range(OWN):
            axis, pairs = STEPS[k][step]
            sent = added(k, start, start + size).astype(bf16)
            arrived.append(lax.ppermute(sent, axis, pairs))
        for k in range(OWN):
            held[k].append(arrived[k])
        start, size = start + size, size // 2
    last = []
    for shift in (1, 2, 3):
        sent = jnp.concatenate(
            [added(k, 28 + shift, 29 + shift).astype(bf16) for k in range(OWN)]
        )
        last.append(lax.ppermute(sent, "zh", shifted(4, shift)))
    rests = [added(k, 28, 29)[0] for k in range(OWN)]
    owned, rows = total(rests, last, devices)
    squares = lax.all_to_all(rows, EVERY, split_axis=0, concat_axis=0, tiled=True)
    sums = [owned] + [lax.ppermute(owned, "expert", shifted(4, s)) for s in (1, 2, 3)]
    squares = squares.reshape(devices, -1)
    outs = finish(numel, mine, step_count, squares, sums, states)
    return (*outs[:8], outs[8].astype(bf16))


def solution(mesh):
    split = Mesh(
        mesh.devices.reshape(4, 4, 2, 2, mesh.shape["expert"]), EVERY
    )
    tiles = P(DP_EXPERT, None, None)
    each = P(DP_EXPERT)
    return jax.shard_map(
        on_device,
        mesh=split,
        in_specs=(
            P(DP, "expert", None, None),
            P("expert", None),
            P(),
            tiles,
            tiles,
            each,
            each,
            tiles,
            each,
            each,
        ),
        out_specs=(
            tiles,
            tiles,
            each,
            each,
            tiles,
            each,
            each,
            P(DP, None, None),
            P(DP),
        ),
        check_vma=False,
    )
```

```python
import jax
import jax.numpy as jnp
from jax import lax
from jax.experimental import pallas as pl
from jax.experimental.pallas import tpu as pltpu
from jax.sharding import Mesh
from jax.sharding import PartitionSpec as P

DP = ("y", "zh", "zl", "core")
Z = ("zh", "zl")
EVERY = ("y", "zh", "zl", "core", "expert")
DP_EXPERT = EVERY

OWN = 4

BETA_ONE = 0.9
BETA_TWO = 0.95
LEARN_RATE = 0.01
WEIGHT_DECAY = 0.1
CLIP_RMS = 0.5
LOG_SPAN = 4.0
EPSILON = 1e-06
ADAM_EPS = 1e-08

VMEM = pltpu.VMEM
SMEM = pltpu.SMEM

Y_EVEN = [(i, i ^ 1) for i in range(4)]
Y_ODD = [(i, i ^ 3) for i in range(4)]
Z_EVEN = [(i, i ^ 1) for i in range(8)]
Z_ODD = [(i, (i + 1) % 8 if i % 2 else (i - 1) % 8) for i in range(8)]

STEPS = (
    (("y", Y_EVEN), (Z, Z_EVEN), ("y", Y_ODD)),
    (("y", Y_ODD), (Z, Z_ODD), ("y", Y_EVEN)),
    ((Z, Z_EVEN), ("y", Y_EVEN), ("y", Y_ODD)),
    ((Z, Z_ODD), ("y", Y_ODD), ("y", Y_EVEN)),
)


def limit(mib):
    return pltpu.CompilerParams(vmem_limit_bytes=mib * 2**20)


def shifted(count, by):
    return [(i, (i + by) % count) for i in range(count)]


def owner_of(k, place, y, zh, zl):
    bits = ((place >> 4) & 1, (place >> 3) & 1, (place >> 2) & 1)
    shift = place & 3
    for bit, (axis, pairs) in zip(bits, STEPS[k]):
        goes = 1 - bit
        if axis == "y":
            y = y ^ (goes * (1 if pairs is Y_EVEN else 3))
        else:
            if pairs is Z_ODD:
                zh = (zh + goes * (2 * zl - 1)) & 3
            zl = zl ^ goes
    return y, (zh + shift) & 3, zl


def pick_kernel(other, table, grads, *outs):
    y, zh, zl = (lax.axis_index(a) for a in DP[:3])
    core = lax.axis_index("core") ^ other
    for k in range(OWN):

        def move(place, _, k=k):
            oy, ozh, ozl = owner_of(k, place, y, zh, zl)
            slot = ((((oy * 4 + ozh) * 2 + ozl) * 2) + core) * OWN + k
            outs[k][place] = grads[table[slot]]
            return 0

        lax.fori_loop(0, outs[k].shape[0], move, 0, unroll=8)


def pick(other, table, grads):
    tile = grads.shape[1:]
    count = grads.shape[0] // (2 * OWN)

    def body(*refs):
        pick_kernel(other, *refs)

    return pl.pallas_call(
        body,
        out_shape=[VMEM((count, *tile), grads.dtype)] * OWN,
        in_specs=[pl.BlockSpec(memory_space=SMEM), pl.BlockSpec(memory_space=VMEM)],
        out_specs=[pl.BlockSpec(memory_space=VMEM)] * OWN,
        compiler_params=limit(2),
        name="pick",
    )(table, grads)


def in_hbm(arrays):
    return [pltpu.with_memory_space_constraint(a, pltpu.HBM) for a in arrays]


def in_vmem(arrays):
    return [pltpu.with_memory_space_constraint(a, VMEM) for a in arrays]


def root(magnitude, power):
    return jnp.exp(jnp.log(magnitude) * power)


def decode_kernel(fs, fp, ss, sp, master, first_code, second_code, out):
    for i in range(OWN):
        out[i] = master[i]
        for base, code, scale, power in ((OWN, first_code, fs, fp), (2 * OWN, second_code, ss, sp)):
            values = code[i].astype(jnp.float32)
            old = scale[i] * root(jnp.abs(values), 1.0 / jnp.full(values.shape, power[i]))
            out[base + i] = jnp.where(values < 0, -old, old)


def decode(fs, fp, ss, sp, master, first_code, second_code):
    return pl.pallas_call(
        decode_kernel,
        out_shape=jax.ShapeDtypeStruct((3 * OWN, *master.shape[1:]), jnp.float32),
        in_specs=[pl.BlockSpec(memory_space=SMEM)] * 4 + [pl.BlockSpec(memory_space=VMEM)] * 3,
        out_specs=pl.BlockSpec(memory_space=VMEM),
        compiler_params=limit(8),
        name="decode",
    )(fs, fp, ss, sp, master, first_code, second_code)


def total_kernel(*refs):
    parts, (owned, rounded, row) = refs[:-3], refs[-3:]
    squares = jnp.zeros((1, owned.shape[-1]), jnp.float32)
    for k in range(OWN):
        total = parts[k][...]
        for received in parts[OWN:]:
            total = total + received[k].astype(jnp.float32)
        owned[k] = total
        rounded[k] = total.astype(rounded.dtype)
        squares = squares + jnp.sum(total * total, axis=0, keepdims=True)
    row[...] = jnp.broadcast_to(squares[None], row.shape)


def total(rests, received, devices):
    tile = rests[0].shape
    return pl.pallas_call(
        total_kernel,
        out_shape=[
            pltpu.HBM((OWN, *tile), jnp.float32),
            pltpu.HBM((OWN, *tile), jnp.bfloat16),
            pltpu.HBM((devices, 1, tile[-1]), jnp.float32),
        ],
        in_specs=[pl.BlockSpec(memory_space=VMEM)] * (len(rests) + len(received)),
        out_specs=[pl.BlockSpec(memory_space=VMEM)] * 3,
        compiler_params=limit(8),
        name="total",
    )(*in_vmem(rests), *in_vmem(received))


def encode(values, code, scales, powers, i):
    absval = jnp.abs(values)
    largest = jnp.max(absval, axis=(0, 1), keepdims=True)
    average = jnp.sum(absval, axis=(0, 1), keepdims=True) / float(values.shape[0] * values.shape[1])
    power = jnp.clip(LOG_SPAN / jnp.log(1.0 + largest / (average + EPSILON)), 1.0, 3.0)
    scale = largest + EPSILON
    coded = root(absval / scale, power)
    code[i] = jnp.where(values < 0, -coded, coded).astype(code.dtype)
    scales[i] = scale[0, 0]
    powers[i] = power[0, 0]


def finish_kernel(numel, step, squares, *refs):
    grads, states = refs[:4], refs[4:8]
    (new_master, fcode, fscale, fpower, scode, sscale, spower, wcode, wscale) = refs[8:]
    f32 = jnp.float32
    total_sq = jnp.sum(squares[...], axis=(0, 1), keepdims=True)
    clip = jnp.minimum(1.0, CLIP_RMS / jnp.sqrt(total_sq / numel + EPSILON))
    steps = jnp.full((1, 1), step[0]).astype(f32)
    bias_one = 1.0 - jnp.exp(steps * jnp.log(jnp.full((1, 1), BETA_ONE, f32)))
    bias_two = 1.0 - jnp.exp(steps * jnp.log(jnp.full((1, 1), BETA_TWO, f32)))
    lane = lax.broadcasted_iota(jnp.int32, wscale.shape, 1)
    scales = jnp.zeros(wscale.shape, f32)
    for shift in range(4):
        base = ((lax.axis_index("expert") - shift) & 3) * OWN
        for k in range(OWN):
            state = states[shift]
            master = state[k]
            grad = grads[shift][k].astype(f32) * clip
            first = BETA_ONE * state[OWN + k] + (1.0 - BETA_ONE) * grad
            second = BETA_TWO * state[2 * OWN + k] + (1.0 - BETA_TWO) * grad * grad
            update = first / bias_one / (jnp.sqrt(second / bias_two) + ADAM_EPS)
            moved = master - LEARN_RATE * (update + WEIGHT_DECAY * master)
            if shift == 0:
                new_master[k] = moved
                encode(first, fcode, fscale, fpower, k)
                encode(second, scode, sscale, spower, k)
            largest = jnp.max(jnp.abs(moved), axis=(0, 1), keepdims=True) + EPSILON
            scale = largest.astype(jnp.bfloat16).astype(f32)
            scales = jnp.where(lane == base + k, scale, scales)
            wcode[base + k] = (moved / scale).astype(wcode.dtype)
    wscale[...] = scales


def finish(numel, step, squares, grads, states):
    tile = grads[0].shape[1:]
    f32, bf16 = jnp.float32, jnp.bfloat16

    def body(*refs):
        finish_kernel(numel, *refs)

    shapes = [
        ((OWN, *tile), f32, VMEM),
        ((OWN, *tile), bf16, VMEM),
        ((OWN,), f32, SMEM),
        ((OWN,), f32, SMEM),
        ((OWN, *tile), bf16, VMEM),
        ((OWN,), f32, SMEM),
        ((OWN,), f32, SMEM),
        ((4 * OWN, *tile), bf16, VMEM),
    ]
    return pl.pallas_call(
        body,
        out_shape=[jax.ShapeDtypeStruct(s, d) for s, d, _ in shapes] + [VMEM((1, 128), f32)],
        in_specs=[pl.BlockSpec(memory_space=SMEM)] + [pl.BlockSpec(memory_space=VMEM)] * 9,
        out_specs=[pl.BlockSpec(memory_space=m) for _, _, m in shapes]
        + [pl.BlockSpec(memory_space=VMEM)],
        compiler_params=limit(24),
        name="finish",
    )(step, *in_vmem([squares]), *in_hbm(grads), *in_vmem(states))


def on_device(
    gradients,
    owner_table,
    step_count,
    master,
    first_code,
    first_scale,
    first_power,
    second_code,
    second_scale,
    second_power,
):
    f32, bf16 = jnp.float32, jnp.bfloat16
    devices = lax.axis_size(EVERY)
    numel = float(devices * master.size)
    table = owner_table[0]
    (grads,) = in_vmem([gradients[0]])

    leaving = pick(1, table, grads)
    from_core = [lax.ppermute(t, "core", [(0, 1), (1, 0)]) for t in leaving]
    kept = pick(0, table, grads)
    held = [[kept[k], from_core[k]] for k in range(OWN)]

    def added(k, start, stop):
        longest = held[k][0].shape[0]
        return sum(
            p[p.shape[0] - longest + start : p.shape[0] - longest + stop].astype(f32)
            for p in held[k]
        )

    def exchanged(streams, start, size):
        parts = [added(k, start, start + size).astype(bf16) for k in streams]
        return parts[0] if len(parts) == 1 else jnp.concatenate(parts)

    for k in range(OWN):
        sent = exchanged((k,), 0, 16)
        held[k].append(lax.ppermute(sent, *STEPS[k][0]))
    state = decode(
        first_scale, first_power, second_scale, second_power, master, first_code, second_code
    )
    states = [state]
    for shift in (1, 2, 3):
        states.append(lax.ppermute(state, "expert", shifted(4, shift)))
    arrived = [lax.ppermute(exchanged((k,), 16, 8), *STEPS[k][1]) for k in range(OWN)]
    for k in range(OWN):
        held[k].append(arrived[k])
    for streams in ((0, 2), (1, 3)):
        both = lax.ppermute(exchanged(streams, 24, 4), *STEPS[streams[0]][2])
        for i, k in enumerate(streams):
            held[k].append(both[4 * i : 4 * i + 4])
    last = []
    for shift in (1, 2, 3):
        sent = jnp.concatenate(
            [added(k, 28 + shift, 29 + shift).astype(bf16) for k in range(OWN)]
        )
        last.append(lax.ppermute(sent, "zh", shifted(4, shift)))
    rests = [added(k, 28, 29)[0] for k in range(OWN)]
    owned, rounded, rows = total(rests, last, devices)
    squares = lax.all_to_all(rows, EVERY, split_axis=0, concat_axis=0, tiled=True)
    sums = [owned]
    for shift in (1, 2, 3):
        sums.append(lax.ppermute(rounded, "expert", shifted(4, shift)))
    outs = finish(numel, step_count, squares.reshape(devices, -1), sums, states)
    return (*outs[:8], outs[8][0, : 4 * OWN].astype(bf16))


def solution(mesh):
    split = Mesh(
        mesh.devices.reshape(4, 4, 2, 2, mesh.shape["expert"]), EVERY
    )
    tiles = P(DP_EXPERT, None, None)
    each = P(DP_EXPERT)
    return jax.shard_map(
        on_device,
        mesh=split,
        in_specs=(
            P(DP, "expert", None, None),
            P("expert", None),
            P(),
            tiles,
            tiles,
            each,
            each,
            tiles,
            each,
            each,
        ),
        out_specs=(
            tiles,
            tiles,
            each,
            each,
            tiles,
            each,
            each,
            P(DP, None, None),
            P(DP),
        ),
        check_vma=False,
    )
```
